32 devices in a mesh: grp: 2 (over y), seq: 4 (over z), head: 2 (over x), sub: 2 (over core).
Axes of the slice: x: 2, y: 2, z: 4, core: 2. Of those that a mesh axis runs over, the one named last changes fastest.
Arguments:
- latents: bfloat16 [8, 256, 1152], P(('grp', 'seq'), ('head', 'sub')), parts along dimension 0, may hold values from -6 to 6
- timestep: int32 [2], P('grp'), parts along dimension 0, may hold values from 0 to 29
- time_table: float32 [30, 3, 1152], replicated, may hold values from -3 to 3
- shift_table: float32 [2, 3, 1152], replicated, may hold values from -2 to 2
- qkv_weight: bfloat16 [2, 1152, 16, 216], P(None, None, ('head', 'sub')), may hold values from -0.1875 to 0.1875
- norm_gains: float32 [2, 2, 72], replicated, may hold values from 0.1 to 1.9
- out_weight: bfloat16 [2, 1152, 1152], P(None, ('head', 'sub')), may hold values from -0.1875 to 0.1875
Outputs:
- mixed: bfloat16 [8, 256, 1152], P(('grp', 'seq'), ('head', 'sub')), parts along dimension 0
The draws below stay inside these ranges and needn't reach their ends.
There are 2 independent parts, one for each index of `grp`. The reference program is written for one: setup_inputs(seed, part) draws one part's arguments, and reference() takes and returns one part's arrays. A program takes and returns all parts, laid end to end along the dimension named above; an argument that names none is the same for every part. Nothing has to cross between parts.
All inputs are finite; a program needn't handle non-finite values.
Results may differ from the reference program's by a relative error of at most 0.0095.
Values may be sent and summed in bfloat16 or wider, within the bound.
A program may use at most 64 MiB of HBM per device.

```python
import jax
import jax.numpy as jnp
from jax import lax

D = 1152
HEADS = 16
HEAD_DIM = 72
STEPS = 30
FRAMES = 4
PIX = 256
N_HEAD = 2
N_SUB = 2


def steps_of(stream_key, shape, split, smallest, largest):
    loudness = 1.0
    for position, parts in split:
        draws = jax.random.uniform(jax.random.fold_in(jax.random.fold_in(stream_key, 6), position), (parts,), jnp.float32, smallest / len(split), largest / len(split))
        loudness = loudness * jnp.repeat(jnp.exp(draws), shape[position] // parts).reshape((-1,) + (1,) * (len(shape) - 1 - position))
    return loudness


def scatter_about(stream_key, shape, scale, reach, shards=(), kind=jnp.bfloat16):
    entries = scale * jax.random.normal(stream_key, shape, jnp.float32)
    if shards:
        entries = entries * steps_of(stream_key, shape, shards, -0.22, 0.18)
    return jnp.clip(entries, -reach, reach).astype(kind)


def setup_inputs(seed: int = 0, part: int = 0) -> dict:
    keys = jax.random.split(jax.random.key(seed), 8)
    own_keys = jax.random.split(jax.random.fold_in(keys[7], part), 8)
    latents = scatter_about(own_keys[0], (FRAMES, PIX, D), 1.0, 6.0, ((0, 4), (1, 4)))
    timestep = jax.random.randint(own_keys[1], (1,), 0, STEPS).astype(jnp.int32)
    time_table = scatter_about(keys[2], (STEPS, 3, D), 0.5, 3.0, (), jnp.float32)
    shift_table = scatter_about(keys[3], (2, 3, D), 0.3, 2.0, (), jnp.float32)
    qkv_weight = scatter_about(keys[4], (2, D, HEADS, 3 * HEAD_DIM), D ** -0.5, 0.1875, ((2, 4),))
    norm_gains = jnp.clip(1.0 + 0.18 * jax.random.normal(keys[5], (2, 2, HEAD_DIM), jnp.float32), 0.1, 1.9)
    out_weight = scatter_about(keys[6], (2, D, D), D ** -0.5, 0.1875, ((1, 4),))
    return {"latents": latents, "timestep": timestep, "time_table": time_table, "shift_table": shift_table, "qkv_weight": qkv_weight, "norm_gains": norm_gains, "out_weight": out_weight}


EPSILON = 1e-06

def modulate(values, shift_row, scale_row):
    widened = values.astype(jnp.float32)
    center = lax.optimization_barrier(jnp.mean(widened, axis=-1, keepdims=True))
    spread = lax.optimization_barrier(jnp.mean(jnp.square(widened - center), axis=-1, keepdims=True))
    normal = (widened - center) * lax.rsqrt(spread + EPSILON)
    return (normal * (1.0 + scale_row) + shift_row).astype(jnp.bfloat16)

def rms_gain(values, gain_row):
    return values * lax.rsqrt(lax.optimization_barrier(jnp.mean(jnp.square(values), axis=-1, keepdims=True)) + EPSILON) * gain_row

def project(normed, weight, gain_pair):
    leading = normed.shape[:-1]
    head_count = weight.shape[1]
    head_dim = weight.shape[2] // 3
    flattened = jnp.dot(normed.reshape(-1, normed.shape[-1]), weight.reshape(weight.shape[0], -1), preferred_element_type=jnp.float32)
    pieces = flattened.reshape(leading + (head_count, 3, head_dim))
    queries = rms_gain(pieces[..., 0, :], gain_pair[0])
    key_part = rms_gain(pieces[..., 1, :], gain_pair[1])
    return jnp.concatenate([queries, key_part, pieces[..., 2, :]], axis=-1).astype(jnp.bfloat16)

def attend(packed):
    head_dim = packed.shape[-1] // 3
    queries = packed[..., :head_dim].astype(jnp.float32)
    key_part = packed[..., head_dim:2 * head_dim].astype(jnp.float32)
    value_part = packed[..., 2 * head_dim:].astype(jnp.float32)
    scores = jnp.einsum('qhd,khd->hqk', queries, key_part) * head_dim ** (-0.5)
    exponent = jnp.exp(scores)
    weights = (exponent / lax.optimization_barrier(jnp.sum(exponent, axis=-1, keepdims=True))).astype(jnp.bfloat16)
    return jnp.einsum('hqk,khd->qhd', weights.astype(jnp.float32), value_part).astype(jnp.bfloat16)

def finish(attended, residual, out_matrix, gate_row):
    flat_rows = attended.reshape(-1, out_matrix.shape[0])
    update = jnp.dot(flat_rows, out_matrix, preferred_element_type=jnp.float32)
    update = update.reshape(residual.shape)
    return (residual.astype(jnp.float32) + gate_row * update).astype(jnp.bfloat16)

def reference(latents, timestep, time_table, shift_table, qkv_weight, norm_gains, out_weight):
    modulation = time_table[timestep[0]][None] + shift_table

    def spatial_frame(frame):
        normed = modulate(frame, modulation[0, 0], modulation[0, 1])
        packed = project(normed, qkv_weight[0], norm_gains[0])
        attended = attend(packed)
        return finish(attended, frame, out_weight[0], modulation[0, 2])
    current = lax.map(spatial_frame, latents)
    frame_count, pixel_count, feature_width = current.shape
    block_count = N_HEAD * N_SUB
    slabs = current.reshape(frame_count, block_count, pixel_count // block_count, feature_width)
    slabs = jnp.moveaxis(slabs, 1, 0)

    def temporal_slab(slab):
        normed = modulate(slab, modulation[1, 0], modulation[1, 1])
        packed = project(normed, qkv_weight[1], norm_gains[1])
        attended = jax.vmap(attend, in_axes=1, out_axes=1)(packed)
        return finish(attended, slab, out_weight[1], modulation[1, 2])
    mixed = lax.map(temporal_slab, slabs)
    mixed = jnp.moveaxis(mixed, 0, 1).reshape(frame_count, pixel_count, feature_width)
    return mixed
```

```python
import functools

import jax
import jax.numpy as jnp
from jax import lax
from jax.experimental import pallas as pl
from jax.experimental.pallas import tpu as pltpu
from jax.sharding import PartitionSpec as P

EPSILON = 1e-06


def modulate(values, shift_row, scale_row):
    widened = values.astype(jnp.float32)
    center = jnp.mean(widened, axis=-1, keepdims=True)
    spread = jnp.mean(jnp.square(widened - center), axis=-1, keepdims=True)
    normal = (widened - center) * lax.rsqrt(spread + EPSILON)
    return (normal * (1.0 + scale_row) + shift_row).astype(jnp.bfloat16)


def rms_gain(values, gain_row):
    return (
        values
        * lax.rsqrt(jnp.mean(jnp.square(values), axis=-1, keepdims=True) + EPSILON)
        * gain_row
    )


def project(normed, weight, gain_pair):
    leading = normed.shape[:-1]
    head_count = weight.shape[1]
    head_dim = weight.shape[2] // 3
    flattened = jnp.dot(
        normed.reshape(-1, normed.shape[-1]),
        weight.reshape(weight.shape[0], -1),
        preferred_element_type=jnp.float32,
    )
    pieces = flattened.reshape(leading + (head_count, 3, head_dim))
    queries = rms_gain(pieces[..., 0, :], gain_pair[0])
    key_part = rms_gain(pieces[..., 1, :], gain_pair[1])
    return jnp.concatenate([queries, key_part, pieces[..., 2, :]], axis=-1).astype(jnp.bfloat16)


def attend(packed):
    head_dim = packed.shape[-1] // 3
    queries = packed[..., :head_dim]
    key_part = packed[..., head_dim : 2 * head_dim]
    value_part = packed[..., 2 * head_dim :]
    count = queries.shape[0]
    block = 512 if count % 512 == 0 else count
    blocks = queries.reshape((count // block, block) + queries.shape[1:])

    def one_block(query_block):
        scores = jnp.einsum(
            "qhd,khd->hqk", query_block, key_part, preferred_element_type=jnp.float32
        ) * head_dim ** (-0.5)
        exponent = jnp.exp(scores)
        weights = (exponent / jnp.sum(exponent, axis=-1, keepdims=True)).astype(jnp.bfloat16)
        return jnp.einsum(
            "hqk,khd->qhd", weights, value_part, preferred_element_type=jnp.float32
        ).astype(jnp.bfloat16)

    result = lax.map(one_block, blocks)
    return result.reshape((count,) + result.shape[2:])


def body(latents, timestep, time_table, shift_table, qkv_weight, norm_gains, out_weight):
    feature_width = latents.shape[2]
    chosen = (jnp.arange(time_table.shape[0]) == timestep[0])[:, None, None]
    shared = jnp.sum(jnp.where(chosen, time_table, 0.0), axis=0)
    modulation = shared[None] + shift_table

    def gathered_heads(normed, layer_index):
        return project(
            lax.all_gather(normed, ("head", "sub"), axis=1, tiled=True),
            qkv_weight[layer_index],
            norm_gains[layer_index],
        )

    def back_to_tokens(attended, layer_index):
        merged = attended.reshape(attended.shape[0], attended.shape[1], -1)
        all_heads = lax.all_to_all(merged, ("head", "sub"), split_axis=1, concat_axis=2, tiled=True)
        row_block = all_heads.reshape(-1, all_heads.shape[-1])
        summed = jnp.dot(
            row_block,
            lax.all_gather(out_weight[layer_index], ("head", "sub"), axis=0, tiled=True),
            preferred_element_type=jnp.float32,
        )
        return summed.reshape(all_heads.shape[0], all_heads.shape[1], feature_width)

    normed = modulate(latents, modulation[0, 0], modulation[0, 1])
    packed = gathered_heads(normed, 0)
    attended = lax.map(attend, packed)
    update = back_to_tokens(attended, 0)
    current = (latents.astype(jnp.float32) + modulation[0, 2] * update).astype(jnp.bfloat16)
    shifted_rows = lax.all_to_all(current, "seq", split_axis=1, concat_axis=0, tiled=True)
    packed = gathered_heads(modulate(shifted_rows, modulation[1, 0], modulation[1, 1]), 1)
    attended = jax.vmap(attend, in_axes=1, out_axes=1)(packed)
    update = back_to_tokens(attended, 1)
    result = (shifted_rows.astype(jnp.float32) + modulation[1, 2] * update).astype(jnp.bfloat16)
    return lax.all_to_all(result, "seq", split_axis=0, concat_axis=1, tiled=True)


MESH = pl.DeviceIdType.MESH


def contract(left, right, left_dim, right_dim):
    return lax.dot_general(
        left,
        right,
        (((left_dim,), (right_dim,)), ((), ())),
        preferred_element_type=jnp.float32,
    )


def normalize(rows, shift_row, scale_row):
    center = jnp.mean(rows, axis=-1, keepdims=True)
    moved = rows - center
    spread = jnp.mean(jnp.square(moved), axis=-1, keepdims=True)
    return (moved * lax.rsqrt(spread + EPSILON) * (1.0 + scale_row) + shift_row).astype(jnp.bfloat16)


def fused_kernel(
    seq_size,
    step_ref,
    lat_hbm,
    time_hbm,
    shift_hbm,
    qkv_hbm,
    gain_hbm,
    proj_hbm,
    out_ref,
    lat,
    time_rows,
    shift_rows,
    gain,
    wq,
    wo,
    g0,
    qkv,
    att,
    part0,
    part1,
    pair_out,
    pair_in,
    cross_out,
    cross_in,
    current,
    seq_out,
    g1,
    back_out,
    back_in,
    load_sem,
    send_sem,
    recv_sem,
):
    grp, seq = lax.axis_index("grp"), lax.axis_index("seq")
    head, sub = lax.axis_index("head"), lax.axis_index("sub")
    sibling = (grp, seq, head, 1 - sub)
    across = (grp, seq, 1 - head, sub)

    def along(r):
        return (grp, lax.rem(seq + r, seq_size), head, sub)

    heads, _, width = wq.shape[1:]
    head_dim = wq.shape[2] // 3
    pixels = lat.shape[1]
    tile = pixels // seq_size
    tokens = 4 * pixels

    far_first = sorted(range(1, seq_size), key=lambda r: -min(r, seq_size - r))
    order = far_first + [0]
    place = {r: i for i, r in enumerate([0] + far_first)}

    loads = []
    for i, (source, target) in enumerate(
        [
            (lat_hbm, lat),
            (time_hbm, time_rows),
            (shift_hbm, shift_rows),
            (gain_hbm, gain),
            (qkv_hbm.at[0], wq.at[0]),
            (proj_hbm.at[0], wo.at[0]),
            (qkv_hbm.at[1], wq.at[1]),
            (proj_hbm.at[1], wo.at[1]),
        ]
    ):
        load = pltpu.make_async_copy(source, target, load_sem.at[i])
        load.start()
        loads.append(load)

    barrier = pltpu.get_barrier_semaphore()
    peers = [sibling, across] + [along(r) for r in range(1, seq_size)]
    for peer in peers:
        pl.semaphore_signal(barrier, inc=1, device_id=peer, device_id_type=MESH)

    started = []

    def send(source, target, device):
        i = len(started)
        copy = pltpu.make_async_remote_copy(
            src_ref=source,
            dst_ref=target,
            send_sem=send_sem.at[i],
            recv_sem=recv_sem.at[i],
            device_id=device,
            device_id_type=MESH,
        )
        copy.start()
        started.append(copy)
        return copy

    for load in loads[:4]:
        load.wait()
    step = step_ref[0]

    def modulation(block, j):
        return time_rows[j, pl.ds(step, 1), :] + shift_rows[j, pl.ds(block, 1), :]

    def chunk_rows(r):
        start = lax.rem(seq + r, seq_size) * tile
        return pl.ds(pl.multiple_of(start, tile), tile)

    shift0, scale0, gate0 = (modulation(0, j) for j in range(3))
    for r in range(seq_size):
        rows = lat[0, chunk_rows(r), :].astype(jnp.float32)
        g0[0, pl.ds(r * tile, tile), :] = normalize(rows, shift0, scale0)

    diagonal = lax.broadcasted_iota(jnp.int32, (head_dim, head_dim), 0) == lax.broadcasted_iota(
        jnp.int32, (head_dim, head_dim), 1
    )

    def gain_column(block, which):
        row = gain[block, pl.ds(which, 1), :]
        return jnp.sum(jnp.where(diagonal, row, 0.0), axis=1, keepdims=True)

    pl.semaphore_wait(barrier, len(peers))

    half = pixels // 2
    halves = [pl.ds(0, half), pl.ds(half, half)]
    cross = [send(g0.at[0, part], g0.at[2, part], across) for part in halves]
    pair = send(g0.at[0], g0.at[1], sibling)

    def project_block(block, values, side):
        lanes = pl.ds(side * (tokens // 2), tokens // 2)
        for h in range(heads):
            flat = contract(wq[block, h], values, 1, 1)
            for j in range(3):
                piece = flat[j * head_dim : (j + 1) * head_dim]
                if j < 2:
                    mean = jnp.mean(jnp.square(piece), axis=0, keepdims=True)
                    piece = piece * lax.rsqrt(mean + EPSILON) * gains[block][j]
                qkv[h, pl.ds(j * head_dim, head_dim), lanes] = piece

    gains = [[gain_column(block, j) for j in range(2)] for block in range(2)]
    loads[4].wait()
    pair.wait_recv()
    project_block(0, g0[0:2].reshape(2 * pixels, width), 0)
    forwarded = []
    for part, copy in zip(halves, cross):
        copy.wait_recv()
        forwarded.append(send(g0.at[2, part], g0.at[3, part], sibling))
    for copy in forwarded:
        copy.wait_recv()
    project_block(0, g0[2:4].reshape(2 * pixels, width), 1)

    scale = head_dim ** (-0.5)
    for h in range(heads):
        queries = qkv[h, 0:head_dim].astype(jnp.bfloat16)
        keys = qkv[h, head_dim : 2 * head_dim].astype(jnp.bfloat16)
        values = qkv[h, 2 * head_dim : 3 * head_dim].astype(jnp.bfloat16)
        exponent = jnp.exp(contract(keys, queries, 0, 0) * scale)
        total = jnp.sum(exponent, axis=0, keepdims=True)
        mixed = contract(values, exponent.astype(jnp.bfloat16), 1, 0)
        att[pl.ds(h * head_dim, head_dim)] = mixed / total

    def reduce_pair(block, part):
        pairs, crosses = {}, {}
        for r in order:
            pair_out[block, r, 0] = part(1, r).astype(jnp.bfloat16)
            pair_out[block, r, 1] = part(3, r).astype(jnp.bfloat16)
            pairs[r] = send(pair_out.at[block, r], pair_in.at[block, r], sibling)
        for r in order:
            pairs[r].wait_recv()
            cross_out[block, r] = (part(2, r) + pair_in[block, r, 1].astype(jnp.float32)).astype(jnp.bfloat16)
            crosses[r] = send(cross_out.at[block, r], cross_in.at[block, r], across)
        return crosses

    def reduced(block, part, crosses, r):
        crosses[r].wait_recv()
        return (
            part(0, r)
            + pair_in[block, r, 0].astype(jnp.float32)
            + cross_in[block, r].astype(jnp.float32)
        )

    loads[5].wait()
    part0[...] = contract(att[...].astype(jnp.bfloat16), wo[0], 0, 0).reshape(part0.shape)

    def first_part(slot, r):
        return part0[slot, r]

    crosses = reduce_pair(0, first_part)
    shift1, scale1, gate1 = (modulation(1, j) for j in range(3))
    moves = {}
    for r in order:
        update = reduced(0, first_part, crosses, r)
        rows = (lat[0, chunk_rows(r), :].astype(jnp.float32) + gate0 * update).astype(jnp.bfloat16)
        current[r] = rows
        normed = normalize(rows.astype(jnp.float32), shift1, scale1)
        if r:
            seq_out[r] = normed
            moves[r] = send(seq_out.at[r], g1.at[place[r], 0], along(r))
        else:
            g1[0, 0] = normed

    loads[6].wait()
    by_place = [0] + far_first
    gathered = []

    def spread(i):
        gathered.append(
            (
                send(g1.at[i, 0], g1.at[i, 2], across),
                send(g1.at[i, 0], g1.at[i, 1], sibling),
            )
        )

    relayed = []

    def relay(i):
        gathered[i][0].wait_recv()
        relayed.append(send(g1.at[i, 2], g1.at[i, 3], sibling))

    middle = seq_size // 2
    spread(0)
    for i in range(1, seq_size):
        moves[by_place[i]].wait_recv()
        spread(i)
        relay(i - 1)

    def ready(places):
        for i in places:
            gathered[i][1].wait_recv()
            relayed[i].wait_recv()

    ready(range(middle))
    project_block(1, g1[0:middle].reshape(2 * pixels, width), 0)
    relay(seq_size - 1)
    ready(range(middle, seq_size))
    project_block(1, g1[middle:seq_size].reshape(2 * pixels, width), 1)

    for h in range(heads):
        queries, keys, values = (
            qkv[h, pl.ds(j * head_dim, head_dim)].astype(jnp.bfloat16).astype(jnp.float32)
            for j in range(3)
        )
        total = jnp.zeros((1, tokens), jnp.float32)
        mixed = jnp.zeros((head_dim, tokens), jnp.float32)
        for r in range(seq_size):
            turn = r * 4 * tile
            turned_keys = pltpu.roll(keys, turn, 1) if r else keys
            turned_values = pltpu.roll(values, turn, 1) if r else values
            exponent = jnp.exp(jnp.sum(queries * turned_keys, axis=0, keepdims=True) * scale)
            total = total + exponent
            mixed = mixed + exponent * turned_values
        att[pl.ds(h * head_dim, head_dim)] = mixed / total

    loads[7].wait()
    part1[...] = contract(att[...].astype(jnp.bfloat16), wo[1], 0, 0).reshape(part1.shape)

    def second_part(slot, r):
        return part1[place[r], slot]

    crosses = reduce_pair(1, second_part)
    returns = {}
    for r in order:
        update = reduced(1, second_part, crosses, r)
        if r:
            back_out[r] = update.astype(jnp.bfloat16)
            returns[r] = send(back_out.at[r], back_in.at[r], along(seq_size - r))
        else:
            rows = current[r].astype(jnp.float32) + gate1 * update
            out_ref[0, chunk_rows(r), :] = rows.astype(jnp.bfloat16)
    for r in far_first:
        returns[r].wait_recv()
        rows = current[r].astype(jnp.float32) + gate1 * back_in[r].astype(jnp.float32)
        out_ref[0, chunk_rows(r), :] = rows.astype(jnp.bfloat16)
    for copy in started:
        copy.wait_send()


def fused_body(seq_size, latents, timestep, time_table, shift_table, qkv_weight, norm_gains, out_weight):
    _, pixels, width = latents.shape
    blocks, _, heads, packed = qkv_weight.shape
    head_dim = packed // 3
    tile = pixels // seq_size
    tokens = 4 * pixels
    copies = 5 + 2 * 2 * seq_size + 2 * (seq_size - 1) + 3 * seq_size
    anywhere = pl.BlockSpec(memory_space=pl.ANY)
    half, full = jnp.bfloat16, jnp.float32
    vmem = pltpu.VMEM
    return pl.pallas_call(
        functools.partial(fused_kernel, seq_size),
        out_shape=jax.ShapeDtypeStruct(latents.shape, half),
        in_specs=[pl.BlockSpec(memory_space=pltpu.SMEM)] + [anywhere] * 6,
        out_specs=pl.BlockSpec(memory_space=pltpu.VMEM),
        scratch_shapes=[
            vmem(latents.shape, half),
            vmem((3, time_table.shape[0], width), full),
            vmem((3, blocks, width), full),
            vmem(norm_gains.shape, full),
            vmem((blocks, heads, packed, width), half),
            vmem(out_weight.shape, half),
            vmem((4, pixels, width), half),
            vmem((heads, packed, tokens), full),
            vmem((heads * head_dim, tokens), full),
            vmem((4, seq_size, tile, width), full),
            vmem((seq_size, 4, tile, width), full),
            vmem((blocks, seq_size, 2, tile, width), half),
            vmem((blocks, seq_size, 2, tile, width), half),
            vmem((blocks, seq_size, tile, width), half),
            vmem((blocks, seq_size, tile, width), half),
            vmem((seq_size, tile, width), half),
            vmem((seq_size, tile, width), half),
            vmem((seq_size, 4, tile, width), half),
            vmem((seq_size, tile, width), half),
            vmem((seq_size, tile, width), half),
            pltpu.SemaphoreType.DMA((8,)),
            pltpu.SemaphoreType.DMA((copies,)),
            pltpu.SemaphoreType.DMA((copies,)),
        ],
        compiler_params=pltpu.CompilerParams(
            collective_id=0, has_side_effects=True, vmem_limit_bytes=48 * 1024 * 1024
        ),
    )(
        timestep,
        latents,
        jnp.transpose(time_table, (1, 0, 2)),
        jnp.transpose(shift_table, (1, 0, 2)),
        jnp.transpose(qkv_weight, (0, 2, 3, 1)),
        norm_gains,
        out_weight,
    )


def chosen_body(mesh, *arrays):
    sizes = mesh.shape
    frames, pixels, _ = arrays[0].shape
    head_dim = arrays[4].shape[3] // 3
    fits = (
        sizes["head"] == 2
        and sizes["sub"] == 2
        and frames == 1
        and sizes["seq"] % 2 == 0
        and pixels % (16 * sizes["seq"]) == 0
        and pixels % 64 == 0
        and head_dim % 8 == 0
    )
    if fits:
        return fused_body(sizes["seq"], *arrays)
    return body(*arrays)


def solution(mesh):
    return jax.shard_map(
        functools.partial(chosen_body, mesh),
        mesh=mesh,
        in_specs=(
            P(("grp", "seq"), ("head", "sub"), None),
            P("grp"),
            P(),
            P(),
            P(None, None, ("head", "sub"), None),
            P(),
            P(None, ("head", "sub"), None),
        ),
        out_specs=P(("grp", "seq"), ("head", "sub"), None),
        check_vma=False,
    )
```

```python
import functools

import jax
import jax.numpy as jnp
from jax import lax
from jax.experimental import pallas as pl
from jax.experimental.pallas import tpu as pltpu
from jax.sharding import PartitionSpec as P

EPSILON = 1e-06


def modulate(values, shift_row, scale_row):
    widened = values.astype(jnp.float32)
    center = jnp.mean(widened, axis=-1, keepdims=True)
    spread = jnp.mean(jnp.square(widened - center), axis=-1, keepdims=True)
    normal = (widened - center) * lax.rsqrt(spread + EPSILON)
    return (normal * (1.0 + scale_row) + shift_row).astype(jnp.bfloat16)


def rms_gain(values, gain_row):
    return (
        values
        * lax.rsqrt(jnp.mean(jnp.square(values), axis=-1, keepdims=True) + EPSILON)
        * gain_row
    )


def project(normed, weight, gain_pair):
    leading = normed.shape[:-1]
    head_count = weight.shape[1]
    head_dim = weight.shape[2] // 3
    flattened = jnp.dot(
        normed.reshape(-1, normed.shape[-1]),
        weight.reshape(weight.shape[0], -1),
        preferred_element_type=jnp.float32,
    )
    pieces = flattened.reshape(leading + (head_count, 3, head_dim))
    queries = rms_gain(pieces[..., 0, :], gain_pair[0])
    key_part = rms_gain(pieces[..., 1, :], gain_pair[1])
    return jnp.concatenate([queries, key_part, pieces[..., 2, :]], axis=-1).astype(jnp.bfloat16)


def attend(packed):
    head_dim = packed.shape[-1] // 3
    queries = packed[..., :head_dim]
    key_part = packed[..., head_dim : 2 * head_dim]
    value_part = packed[..., 2 * head_dim :]
    count = queries.shape[0]
    block = 512 if count % 512 == 0 else count
    blocks = queries.reshape((count // block, block) + queries.shape[1:])

    def one_block(query_block):
        scores = jnp.einsum(
            "qhd,khd->hqk", query_block, key_part, preferred_element_type=jnp.float32
        ) * head_dim ** (-0.5)
        exponent = jnp.exp(scores)
        weights = (exponent / jnp.sum(exponent, axis=-1, keepdims=True)).astype(jnp.bfloat16)
        return jnp.einsum(
            "hqk,khd->qhd", weights, value_part, preferred_element_type=jnp.float32
        ).astype(jnp.bfloat16)

    result = lax.map(one_block, blocks)
    return result.reshape((count,) + result.shape[2:])


def body(latents, timestep, time_table, shift_table, qkv_weight, norm_gains, out_weight):
    feature_width = latents.shape[2]
    chosen = (jnp.arange(time_table.shape[0]) == timestep[0])[:, None, None]
    shared = jnp.sum(jnp.where(chosen, time_table, 0.0), axis=0)
    modulation = shared[None] + shift_table

    def gathered_heads(normed, layer_index):
        return project(
            lax.all_gather(normed, ("head", "sub"), axis=1, tiled=True),
            qkv_weight[layer_index],
            norm_gains[layer_index],
        )

    def back_to_tokens(attended, layer_index):
        merged = attended.reshape(attended.shape[0], attended.shape[1], -1)
        all_heads = lax.all_to_all(merged, ("head", "sub"), split_axis=1, concat_axis=2, tiled=True)
        row_block = all_heads.reshape(-1, all_heads.shape[-1])
        summed = jnp.dot(
            row_block,
            lax.all_gather(out_weight[layer_index], ("head", "sub"), axis=0, tiled=True),
            preferred_element_type=jnp.float32,
        )
        return summed.reshape(all_heads.shape[0], all_heads.shape[1], feature_width)

    normed = modulate(latents, modulation[0, 0], modulation[0, 1])
    packed = gathered_heads(normed, 0)
    attended = lax.map(attend, packed)
    update = back_to_tokens(attended, 0)
    current = (latents.astype(jnp.float32) + modulation[0, 2] * update).astype(jnp.bfloat16)
    shifted_rows = lax.all_to_all(current, "seq", split_axis=1, concat_axis=0, tiled=True)
    packed = gathered_heads(modulate(shifted_rows, modulation[1, 0], modulation[1, 1]), 1)
    attended = jax.vmap(attend, in_axes=1, out_axes=1)(packed)
    update = back_to_tokens(attended, 1)
    result = (shifted_rows.astype(jnp.float32) + modulation[1, 2] * update).astype(jnp.bfloat16)
    return lax.all_to_all(result, "seq", split_axis=0, concat_axis=1, tiled=True)


MESH = pl.DeviceIdType.MESH


def contract(left, right, left_dim, right_dim):
    return lax.dot_general(
        left,
        right,
        (((left_dim,), (right_dim,)), ((), ())),
        preferred_element_type=jnp.float32,
    )


def normalize(rows, shift_row, scale_row):
    center = jnp.mean(rows, axis=-1, keepdims=True)
    moved = rows - center
    spread = jnp.mean(jnp.square(moved), axis=-1, keepdims=True)
    return (moved * lax.rsqrt(spread + EPSILON) * (1.0 + scale_row) + shift_row).astype(jnp.bfloat16)


def fused_kernel(
    seq_size,
    step_ref,
    lat_hbm,
    time_hbm,
    shift_hbm,
    qkv_hbm,
    gain_hbm,
    proj_hbm,
    out_ref,
    lat,
    time_rows,
    shift_rows,
    gain,
    wq,
    wo,
    g0,
    qkv,
    att,
    part0,
    part1,
    pair_out,
    pair_in,
    cross_out,
    cross_in,
    current,
    seq_out,
    g1,
    back_out,
    back_in,
    load_sem,
    send_sem,
    recv_sem,
):
    grp, seq = lax.axis_index("grp"), lax.axis_index("seq")
    head, sub = lax.axis_index("head"), lax.axis_index("sub")
    sibling = (grp, seq, head, 1 - sub)
    across = (grp, seq, 1 - head, sub)

    def along(r):
        return (grp, lax.rem(seq + r, seq_size), head, sub)

    heads, _, width = wq.shape[1:]
    head_dim = wq.shape[2] // 3
    pixels = lat.shape[1]
    tile = pixels // seq_size
    tokens = 4 * pixels

    far_first = sorted(range(1, seq_size), key=lambda r: -min(r, seq_size - r))
    order = far_first + [0]
    place = {r: i for i, r in enumerate([0] + far_first)}

    loads = []
    for i, (source, target) in enumerate(
        [
            (lat_hbm, lat),
            (time_hbm, time_rows),
            (shift_hbm, shift_rows),
            (gain_hbm, gain),
            (qkv_hbm.at[0], wq.at[0]),
            (proj_hbm.at[0], wo.at[0]),
            (qkv_hbm.at[1], wq.at[1]),
            (proj_hbm.at[1], wo.at[1]),
        ]
    ):
        load = pltpu.make_async_copy(source, target, load_sem.at[i])
        load.start()
        loads.append(load)

    barrier = pltpu.get_barrier_semaphore()
    peers = [sibling, across] + [along(r) for r in range(1, seq_size)]
    for peer in peers:
        pl.semaphore_signal(barrier, inc=1, device_id=peer, device_id_type=MESH)

    started = []

    def send(source, target, device):
        i = len(started)
        copy = pltpu.make_async_remote_copy(
            src_ref=source,
            dst_ref=target,
            send_sem=send_sem.at[i],
            recv_sem=recv_sem.at[i],
            device_id=device,
            device_id_type=MESH,
        )
        copy.start()
        started.append(copy)
        return copy

    for load in loads[:4]:
        load.wait()
    step = step_ref[0]

    def modulation(block, j):
        return time_rows[j, pl.ds(step, 1), :] + shift_rows[j, pl.ds(block, 1), :]

    def chunk_rows(r):
        start = lax.rem(seq + r, seq_size) * tile
        return pl.ds(pl.multiple_of(start, tile), tile)

    shift0, scale0, gate0 = (modulation(0, j) for j in range(3))
    for r in range(seq_size):
        rows = lat[0, chunk_rows(r), :].astype(jnp.float32)
        g0[0, pl.ds(r * tile, tile), :] = normalize(rows, shift0, scale0)

    diagonal = lax.broadcasted_iota(jnp.int32, (head_dim, head_dim), 0) == lax.broadcasted_iota(
        jnp.int32, (head_dim, head_dim), 1
    )

    def gain_column(block, which):
        row = gain[block, pl.ds(which, 1), :]
        return jnp.sum(jnp.where(diagonal, row, 0.0), axis=1, keepdims=True)

    pl.semaphore_wait(barrier, len(peers))

    half = pixels // 2
    halves = [pl.ds(0, half), pl.ds(half, half)]
    cross = [send(g0.at[0, part], g0.at[2, part], across) for part in halves]
    pair = send(g0.at[0], g0.at[1], sibling)

    def project_block(block, values, side):
        lanes = pl.ds(side * (tokens // 2), tokens // 2)
        for h in range(heads):
            flat = contract(wq[block, h], values, 1, 1)
            for j in range(3):
                piece = flat[j * head_dim : (j + 1) * head_dim]
                if j < 2:
                    mean = jnp.mean(jnp.square(piece), axis=0, keepdims=True)
                    piece = piece * lax.rsqrt(mean + EPSILON) * gains[block][j]
                qkv[h, pl.ds(j * head_dim, head_dim), lanes] = piece

    gains = [[gain_column(block, j) for j in range(2)] for block in range(2)]
    loads[4].wait()
    pair.wait_recv()
    project_block(0, g0[0:2].reshape(2 * pixels, width), 0)
    forwarded = []
    for part, copy in zip(halves, cross):
        copy.wait_recv()
        forwarded.append(send(g0.at[2, part], g0.at[3, part], sibling))
    for copy in forwarded:
        copy.wait_recv()
    project_block(0, g0[2:4].reshape(2 * pixels, width), 1)

    scale = head_dim ** (-0.5)
    for h in range(heads):
        queries = qkv[h, 0:head_dim].astype(jnp.bfloat16)
        keys = qkv[h, head_dim : 2 * head_dim].astype(jnp.bfloat16)
        values = qkv[h, 2 * head_dim : 3 * head_dim].astype(jnp.bfloat16)
        exponent = jnp.exp(contract(keys, queries, 0, 0) * scale)
        total = jnp.sum(exponent, axis=0, keepdims=True)
        mixed = contract(values, exponent.astype(jnp.bfloat16), 1, 0)
        att[pl.ds(h * head_dim, head_dim)] = mixed / total

    def reduce_pair(block, part):
        pairs, crosses = {}, {}
        for r in order:
            pair_out[block, r, 0] = part(1, r).astype(jnp.bfloat16)
            pair_out[block, r, 1] = part(3, r).astype(jnp.bfloat16)
            pairs[r] = send(pair_out.at[block, r], pair_in.at[block, r], sibling)
        for r in order:
            pairs[r].wait_recv()
            cross_out[block, r] = (part(2, r) + pair_in[block, r, 1].astype(jnp.float32)).astype(jnp.bfloat16)
            crosses[r] = send(cross_out.at[block, r], cross_in.at[block, r], across)
        return crosses

    def reduced(block, part, crosses, r):
        crosses[r].wait_recv()
        return (
            part(0, r)
            + pair_in[block, r, 0].astype(jnp.float32)
            + cross_in[block, r].astype(jnp.float32)
        )

    loads[5].wait()
    part0[...] = contract(att[...].astype(jnp.bfloat16), wo[0], 0, 0).reshape(part0.shape)

    def first_part(slot, r):
        return part0[slot, r]

    crosses = reduce_pair(0, first_part)
    shift1, scale1, gate1 = (modulation(1, j) for j in range(3))
    moves = {}
    for r in order:
        update = reduced(0, first_part, crosses, r)
        rows = (lat[0, chunk_rows(r), :].astype(jnp.float32) + gate0 * update).astype(jnp.bfloat16)
        current[r] = rows
        normed = normalize(rows.astype(jnp.float32), shift1, scale1)
        if r:
            seq_out[r] = normed
            moves[r] = send(seq_out.at[r], g1.at[place[r], 0], along(r))
        else:
            g1[0, 0] = normed

    loads[6].wait()
    by_place = [0] + far_first
    gathered = []

    def spread(i):
        gathered.append(
            (
                send(g1.at[i, 0], g1.at[i, 2], across),
                send(g1.at[i, 0], g1.at[i, 1], sibling),
            )
        )

    relayed = []

    def relay(i):
        gathered[i][0].wait_recv()
        relayed.append(send(g1.at[i, 2], g1.at[i, 3], sibling))

    middle = seq_size // 2
    spread(0)
    for i in range(1, seq_size):
        moves[by_place[i]].wait_recv()
        spread(i)
        relay(i - 1)

    def ready(places):
        for i in places:
            gathered[i][1].wait_recv()
            relayed[i].wait_recv()

    ready(range(middle))
    project_block(1, g1[0:middle].reshape(2 * pixels, width), 0)
    relay(seq_size - 1)
    ready(range(middle, seq_size))
    project_block(1, g1[middle:seq_size].reshape(2 * pixels, width), 1)

    for h in range(heads):
        queries, keys, values = (
            qkv[h, pl.ds(j * head_dim, head_dim)].astype(jnp.bfloat16).astype(jnp.float32)
            for j in range(3)
        )
        total = jnp.zeros((1, tokens), jnp.float32)
        mixed = jnp.zeros((head_dim, tokens), jnp.float32)
        for r in range(seq_size):
            turn = r * 4 * tile
            turned_keys = pltpu.roll(keys, turn, 1) if r else keys
            turned_values = pltpu.roll(values, turn, 1) if r else values
            exponent = jnp.exp(jnp.sum(queries * turned_keys, axis=0, keepdims=True) * scale)
            total = total + exponent
            mixed = mixed + exponent * turned_values
        att[pl.ds(h * head_dim, head_dim)] = mixed / total

    loads[7].wait()
    part1[...] = contract(att[...].astype(jnp.bfloat16), wo[1], 0, 0).reshape(part1.shape)

    def second_part(slot, r):
        return part1[place[r], slot]

    crosses = reduce_pair(1, second_part)
    returns = {}
    for r in order:
        update = reduced(1, second_part, crosses, r)
        if r:
            back_out[r] = update.astype(jnp.bfloat16)
            returns[r] = send(back_out.at[r], back_in.at[r], along(seq_size - r))
        else:
            rows = current[r].astype(jnp.float32) + gate1 * update
            out_ref[0, chunk_rows(r), :] = rows.astype(jnp.bfloat16)
    for r in far_first:
        returns[r].wait_recv()
        rows = current[r].astype(jnp.float32) + gate1 * back_in[r].astype(jnp.float32)
        out_ref[0, chunk_rows(r), :] = rows.astype(jnp.bfloat16)
    for copy in started:
        copy.wait_send()


def fused_body(seq_size, latents, timestep, time_table, shift_table, qkv_weight, norm_gains, out_weight):
    _, pixels, width = latents.shape
    blocks, _, heads, packed = qkv_weight.shape
    head_dim = packed // 3
    tile = pixels // seq_size
    tokens = 4 * pixels
    copies = 5 + 2 * 2 * seq_size + 2 * (seq_size - 1) + 3 * seq_size
    anywhere = pl.BlockSpec(memory_space=pl.ANY)
    half, full = jnp.bfloat16, jnp.float32
    vmem = pltpu.VMEM
    return pl.pallas_call(
        functools.partial(fused_kernel, seq_size),
        out_shape=jax.ShapeDtypeStruct(latents.shape, half),
        in_specs=[pl.BlockSpec(memory_space=pltpu.SMEM)] + [anywhere] * 6,
        out_specs=pl.BlockSpec(memory_space=pltpu.VMEM),
        scratch_shapes=[
            vmem(latents.shape, half),
            vmem((3, time_table.shape[0], width), full),
            vmem((3, blocks, width), full),
            vmem(norm_gains.shape, full),
            vmem((blocks, heads, packed, width), half),
            vmem(out_weight.shape, half),
            vmem((4, pixels, width), half),
            vmem((heads, packed, tokens), full),
            vmem((heads * head_dim, tokens), full),
            vmem((4, seq_size, tile, width), full),
            vmem((seq_size, 4, tile, width), full),
            vmem((blocks, seq_size, 2, tile, width), half),
            vmem((blocks, seq_size, 2, tile, width), half),
            vmem((blocks, seq_size, tile, width), half),
            vmem((blocks, seq_size, tile, width), half),
            vmem((seq_size, tile, width), half),
            vmem((seq_size, tile, width), half),
            vmem((seq_size, 4, tile, width), half),
            vmem((seq_size, tile, width), half),
            vmem((seq_size, tile, width), half),
            pltpu.SemaphoreType.DMA((8,)),
            pltpu.SemaphoreType.DMA((copies,)),
            pltpu.SemaphoreType.DMA((copies,)),
        ],
        compiler_params=pltpu.CompilerParams(
            collective_id=0, has_side_effects=True, vmem_limit_bytes=67_043_328
        ),
    )(
        timestep,
        latents,
        jnp.transpose(time_table, (1, 0, 2)),
        jnp.transpose(shift_table, (1, 0, 2)),
        jnp.transpose(qkv_weight, (0, 2, 3, 1)),
        norm_gains,
        out_weight,
    )


def chosen_body(mesh, *arrays):
    sizes = mesh.shape
    frames, pixels, _ = arrays[0].shape
    head_dim = arrays[4].shape[3] // 3
    fits = (
        sizes["head"] == 2
        and sizes["sub"] == 2
        and frames == 1
        and sizes["seq"] % 2 == 0
        and pixels % (16 * sizes["seq"]) == 0
        and pixels % 64 == 0
        and head_dim % 8 == 0
    )
    if fits:
        return fused_body(sizes["seq"], *arrays)
    return body(*arrays)


def solution(mesh):
    return jax.shard_map(
        functools.partial(chosen_body, mesh),
        mesh=mesh,
        in_specs=(
            P(("grp", "seq"), ("head", "sub"), None),
            P("grp"),
            P(),
            P(),
            P(None, None, ("head", "sub"), None),
            P(),
            P(None, ("head", "sub"), None),
        ),
        out_specs=P(("grp", "seq"), ("head", "sub"), None),
        check_vma=False,
    )
```

```python
import functools

import jax
import jax.numpy as jnp
from jax import lax
from jax.experimental import pallas as pl
from jax.experimental.pallas import tpu as pltpu
from jax.sharding import PartitionSpec as P

EPSILON = 1e-06


def modulate(values, shift_row, scale_row):
    widened = values.astype(jnp.float32)
    center = jnp.mean(widened, axis=-1, keepdims=True)
    spread = jnp.mean(jnp.square(widened - center), axis=-1, keepdims=True)
    normal = (widened - center) * lax.rsqrt(spread + EPSILON)
    return (normal * (1.0 + scale_row) + shift_row).astype(jnp.bfloat16)


def rms_gain(values, gain_row):
    return (
        values
        * lax.rsqrt(jnp.mean(jnp.square(values), axis=-1, keepdims=True) + EPSILON)
        * gain_row
    )


def project(normed, weight, gain_pair):
    leading = normed.shape[:-1]
    head_count = weight.shape[1]
    head_dim = weight.shape[2] // 3
    flattened = jnp.dot(
        normed.reshape(-1, normed.shape[-1]),
        weight.reshape(weight.shape[0], -1),
        preferred_element_type=jnp.float32,
    )
    pieces = flattened.reshape(leading + (head_count, 3, head_dim))
    queries = rms_gain(pieces[..., 0, :], gain_pair[0])
    key_part = rms_gain(pieces[..., 1, :], gain_pair[1])
    return jnp.concatenate([queries, key_part, pieces[..., 2, :]], axis=-1).astype(jnp.bfloat16)


def attend(packed):
    head_dim = packed.shape[-1] // 3
    queries = packed[..., :head_dim]
    key_part = packed[..., head_dim : 2 * head_dim]
    value_part = packed[..., 2 * head_dim :]
    count = queries.shape[0]
    block = 512 if count % 512 == 0 else count
    blocks = queries.reshape((count // block, block) + queries.shape[1:])

    def one_block(query_block):
        scores = jnp.einsum(
            "qhd,khd->hqk", query_block, key_part, preferred_element_type=jnp.float32
        ) * head_dim ** (-0.5)
        exponent = jnp.exp(scores)
        weights = (exponent / jnp.sum(exponent, axis=-1, keepdims=True)).astype(jnp.bfloat16)
        return jnp.einsum(
            "hqk,khd->qhd", weights, value_part, preferred_element_type=jnp.float32
        ).astype(jnp.bfloat16)

    result = lax.map(one_block, blocks)
    return result.reshape((count,) + result.shape[2:])


def body(latents, timestep, time_table, shift_table, qkv_weight, norm_gains, out_weight):
    feature_width = latents.shape[2]
    chosen = (jnp.arange(time_table.shape[0]) == timestep[0])[:, None, None]
    shared = jnp.sum(jnp.where(chosen, time_table, 0.0), axis=0)
    modulation = shared[None] + shift_table

    def gathered_heads(normed, layer_index):
        return project(
            lax.all_gather(normed, ("head", "sub"), axis=1, tiled=True),
            qkv_weight[layer_index],
            norm_gains[layer_index],
        )

    def back_to_tokens(attended, layer_index):
        merged = attended.reshape(attended.shape[0], attended.shape[1], -1)
        all_heads = lax.all_to_all(merged, ("head", "sub"), split_axis=1, concat_axis=2, tiled=True)
        row_block = all_heads.reshape(-1, all_heads.shape[-1])
        summed = jnp.dot(
            row_block,
            lax.all_gather(out_weight[layer_index], ("head", "sub"), axis=0, tiled=True),
            preferred_element_type=jnp.float32,
        )
        return summed.reshape(all_heads.shape[0], all_heads.shape[1], feature_width)

    normed = modulate(latents, modulation[0, 0], modulation[0, 1])
    packed = gathered_heads(normed, 0)
    attended = lax.map(attend, packed)
    update = back_to_tokens(attended, 0)
    current = (latents.astype(jnp.float32) + modulation[0, 2] * update).astype(jnp.bfloat16)
    shifted_rows = lax.all_to_all(current, "seq", split_axis=1, concat_axis=0, tiled=True)
    packed = gathered_heads(modulate(shifted_rows, modulation[1, 0], modulation[1, 1]), 1)
    attended = jax.vmap(attend, in_axes=1, out_axes=1)(packed)
    update = back_to_tokens(attended, 1)
    result = (shifted_rows.astype(jnp.float32) + modulation[1, 2] * update).astype(jnp.bfloat16)
    return lax.all_to_all(result, "seq", split_axis=0, concat_axis=1, tiled=True)


MESH = pl.DeviceIdType.MESH


def contract(left, right, left_dim, right_dim):
    return lax.dot_general(
        left,
        right,
        (((left_dim,), (right_dim,)), ((), ())),
        preferred_element_type=jnp.float32,
    )


def normalize(rows, shift_row, scale_row):
    center = jnp.mean(rows, axis=-1, keepdims=True)
    moved = rows - center
    spread = jnp.mean(jnp.square(moved), axis=-1, keepdims=True)
    return (moved * lax.rsqrt(spread + EPSILON) * (1.0 + scale_row) + shift_row).astype(jnp.bfloat16)


def fused_kernel(
    seq_size,
    step_hbm,
    lat_hbm,
    time_hbm,
    shift_hbm,
    qkv_hbm,
    gain_hbm,
    proj_hbm,
    out_ref,
    step_ref,
    lat,
    time_rows,
    shift_rows,
    gain,
    wq,
    wo,
    g0,
    qkv,
    att,
    part0,
    part1,
    pair0_out,
    pair0_in,
    pair1_out,
    pair1_in,
    cross_out,
    cross_in,
    current,
    seq_out,
    g1,
    back_out,
    back_in,
    load_sem,
    send_sem,
    recv_sem,
):
    grp, seq = lax.axis_index("grp"), lax.axis_index("seq")
    head, sub = lax.axis_index("head"), lax.axis_index("sub")
    sibling = (grp, seq, head, 1 - sub)
    across = (grp, seq, 1 - head, sub)

    def partner(r):
        position = seq
        bit = 1
        while bit < seq_size:
            if r & bit:
                position = position + bit - 2 * bit * lax.rem(lax.div(seq, bit), 2)
            bit *= 2
        return position

    def along(r):
        return (grp, partner(r), head, sub)

    heads, _, width = wq.shape[1:]
    head_dim = wq.shape[2] // 3
    pixels = lat.shape[1]
    tile = pixels // seq_size
    tokens = 4 * pixels

    far_first = list(range(seq_size - 1, 0, -1))
    order = far_first + [0]
    place = {r: i for i, r in enumerate([0] + far_first)}

    loads = []
    for i, (source, target) in enumerate(
        [
            (lat_hbm, lat),
            (time_hbm, time_rows),
            (shift_hbm, shift_rows),
            (gain_hbm, gain),
            (qkv_hbm.at[0], wq.at[0]),
            (proj_hbm.at[0], wo.at[0]),
            (qkv_hbm.at[1], wq.at[1]),
            (proj_hbm.at[1], wo.at[1]),
            (step_hbm, step_ref),
        ]
    ):
        load = pltpu.make_async_copy(source, target, load_sem.at[i])
        load.start()
        loads.append(load)

    barrier = pltpu.get_barrier_semaphore()
    peers = [sibling, across] + [along(r) for r in range(1, seq_size)]
    for peer in peers:
        pl.semaphore_signal(barrier, inc=1, device_id=peer, device_id_type=MESH)

    started = []

    def send(source, target, device):
        i = len(started)
        copy = pltpu.make_async_remote_copy(
            src_ref=source,
            dst_ref=target,
            send_sem=send_sem.at[i],
            recv_sem=recv_sem.at[i],
            device_id=device,
            device_id_type=MESH,
        )
        copy.start()
        started.append(copy)
        return copy

    for load in loads[:4] + loads[8:]:
        load.wait()
    step = step_ref[0]

    def modulation(block, j):
        return time_rows[j, pl.ds(step, 1), :] + shift_rows[j, pl.ds(block, 1), :]

    def chunk_rows(r):
        start = partner(r) * tile
        return pl.ds(pl.multiple_of(start, tile), tile)

    shift0, scale0, gate0 = (modulation(0, j) for j in range(3))
    for r in range(seq_size):
        rows = lat[0, chunk_rows(r), :].astype(jnp.float32)
        g0[0, pl.ds(r * tile, tile), :] = normalize(rows, shift0, scale0)

    diagonal = lax.broadcasted_iota(jnp.int32, (head_dim, head_dim), 0) == lax.broadcasted_iota(
        jnp.int32, (head_dim, head_dim), 1
    )

    def gain_column(block, which):
        row = gain[block, pl.ds(which, 1), :]
        return jnp.sum(jnp.where(diagonal, row, 0.0), axis=1, keepdims=True)

    pl.semaphore_wait(barrier, len(peers))

    half = pixels // 2
    halves = [pl.ds(0, half), pl.ds(half, half)]
    cross = [send(g0.at[0, part], g0.at[2, part], across) for part in halves]
    pair = send(g0.at[0], g0.at[1], sibling)

    def project_block(block, values, side):
        lanes = pl.ds(side * (tokens // 2), tokens // 2)
        for h in range(heads):
            flat = contract(wq[block, h], values, 1, 1)
            for j in range(3):
                piece = flat[j * head_dim : (j + 1) * head_dim]
                if j < 2:
                    mean = jnp.mean(jnp.square(piece), axis=0, keepdims=True)
                    piece = piece * lax.rsqrt(mean + EPSILON) * gains[block][j]
                qkv[h, pl.ds(j * head_dim, head_dim), lanes] = piece

    gains = [[gain_column(block, j) for j in range(2)] for block in range(2)]
    loads[4].wait()
    pair.wait_recv()
    project_block(0, g0[0:2].reshape(2 * pixels, width), 0)
    forwarded = []
    for part, copy in zip(halves, cross):
        copy.wait_recv()
        forwarded.append(send(g0.at[2, part], g0.at[3, part], sibling))
    for copy in forwarded:
        copy.wait_recv()
    project_block(0, g0[2:4].reshape(2 * pixels, width), 1)

    scale = head_dim ** (-0.5)

    for h in range(heads):
        queries = qkv[h, 0:head_dim].astype(jnp.bfloat16)
        keys = qkv[h, head_dim : 2 * head_dim].astype(jnp.bfloat16)
        values = qkv[h, 2 * head_dim : 3 * head_dim].astype(jnp.bfloat16)
        exponent = jnp.exp(contract(keys, queries, 0, 0) * scale)
        total = jnp.sum(exponent, axis=0, keepdims=True)
        mixed = contract(values, exponent.astype(jnp.bfloat16), 1, 0)
        att[pl.ds(h * head_dim, head_dim)] = mixed / total

    def project_out(block, side, part):
        lanes = pl.ds(side * (tokens // 2), tokens // 2)
        partial = contract(att[:, lanes].astype(jnp.bfloat16), wo[block], 0, 0)
        first = side * (part.shape[0] // 2)
        part[pl.ds(first, part.shape[0] // 2)] = partial.reshape(
            (part.shape[0] // 2,) + part.shape[1:]
        )

    loads[5].wait()
    project_out(0, 1, part0)
    far_pairs = {}
    for r in order:
        pair0_out[1, r] = part0[3, r].astype(jnp.bfloat16)
        far_pairs[r] = send(pair0_out.at[1, r], pair0_in.at[1, r], sibling)
    project_out(0, 0, part0)
    pair0_out[0] = part0[1].astype(jnp.bfloat16)
    near_pair = send(pair0_out.at[0], pair0_in.at[0], sibling)
    crosses = {}
    for r in order:
        far_pairs[r].wait_recv()
        summed = part0[2, r] + pair0_in[1, r].astype(jnp.float32)
        cross_out[0, r] = summed.astype(jnp.bfloat16)
        crosses[r] = send(cross_out.at[0, r], cross_in.at[0, r], across)
    near_pair.wait_recv()
    shift1, scale1, gate1 = (modulation(1, j) for j in range(3))
    moves = {}
    for r in order:
        crosses[r].wait_recv()
        update = (
            part0[0, r]
            + pair0_in[0, r].astype(jnp.float32)
            + cross_in[0, r].astype(jnp.float32)
        )
        rows = (lat[0, chunk_rows(r), :].astype(jnp.float32) + gate0 * update).astype(jnp.bfloat16)
        current[r] = rows
        normed = normalize(rows.astype(jnp.float32), shift1, scale1)
        if r:
            seq_out[r] = normed
            moves[r] = send(seq_out.at[r], g1.at[place[r], 0], along(r))
        else:
            g1[0, 0] = normed

    loads[6].wait()
    by_place = [0] + far_first
    gathered = []

    def spread(i):
        gathered.append(
            (
                send(g1.at[i, 0], g1.at[i, 2], across),
                send(g1.at[i, 0], g1.at[i, 1], sibling),
            )
        )

    relayed = []

    def relay(i):
        gathered[i][0].wait_recv()
        relayed.append(send(g1.at[i, 2], g1.at[i, 3], sibling))

    middle = seq_size // 2
    spread(0)
    for i in range(1, seq_size):
        moves[by_place[i]].wait_recv()
        spread(i)
    for i in range(seq_size - 1):
        relay(i)

    def ready(places):
        for i in places:
            gathered[i][1].wait_recv()
            relayed[i].wait_recv()

    ready(range(middle))
    project_block(1, g1[0:middle].reshape(2 * pixels, width), 0)
    relay(seq_size - 1)
    ready(range(middle, seq_size))
    project_block(1, g1[middle:seq_size].reshape(2 * pixels, width), 1)

    for h in range(heads):
        queries, keys, values = (
            qkv[h, pl.ds(j * head_dim, head_dim)].astype(jnp.bfloat16).astype(jnp.float32)
            for j in range(3)
        )
        total = jnp.zeros((1, tokens), jnp.float32)
        mixed = jnp.zeros((head_dim, tokens), jnp.float32)
        for r in range(seq_size):
            turn = r * 4 * tile
            turned_keys = pltpu.roll(keys, turn, 1) if r else keys
            turned_values = pltpu.roll(values, turn, 1) if r else values
            exponent = jnp.exp(jnp.sum(queries * turned_keys, axis=0, keepdims=True) * scale)
            total = total + exponent
            mixed = mixed + exponent * turned_values
        att[pl.ds(h * head_dim, head_dim)] = mixed / total

    loads[7].wait()
    pairs, crosses = {}, {}
    for side in range(2):
        project_out(1, side, part1)
        for i in range(side * middle, (side + 1) * middle):
            r = by_place[i]
            pair1_out[r, 0] = part1[i, 1].astype(jnp.bfloat16)
            pair1_out[r, 1] = part1[i, 3].astype(jnp.bfloat16)
            pairs[r] = send(pair1_out.at[r], pair1_in.at[r], sibling)
    for r in order:
        pairs[r].wait_recv()
        summed = part1[place[r], 2] + pair1_in[r, 1].astype(jnp.float32)
        cross_out[1, r] = summed.astype(jnp.bfloat16)
        crosses[r] = send(cross_out.at[1, r], cross_in.at[1, r], across)
    returns = {}
    for r in order:
        crosses[r].wait_recv()
        update = (
            part1[place[r], 0]
            + pair1_in[r, 0].astype(jnp.float32)
            + cross_in[1, r].astype(jnp.float32)
        )
        if r:
            back_out[r] = update.astype(jnp.bfloat16)
            returns[r] = send(back_out.at[r], back_in.at[r], along(r))
        else:
            rows = current[r].astype(jnp.float32) + gate1 * update
            out_ref[0, chunk_rows(r), :] = rows.astype(jnp.bfloat16)
    for r in far_first:
        returns[r].wait_recv()
        rows = current[r].astype(jnp.float32) + gate1 * back_in[r].astype(jnp.float32)
        out_ref[0, chunk_rows(r), :] = rows.astype(jnp.bfloat16)
    for copy in started:
        copy.wait_send()


def fused_body(seq_size, latents, timestep, time_table, shift_table, qkv_weight, norm_gains, out_weight):
    _, pixels, width = latents.shape
    blocks, _, heads, packed = qkv_weight.shape
    head_dim = packed // 3
    tile = pixels // seq_size
    tokens = 4 * pixels
    copies = 6 + 4 * seq_size + 2 * (seq_size - 1) + 3 * seq_size
    anywhere = pl.BlockSpec(memory_space=pl.ANY)
    half, full = jnp.bfloat16, jnp.float32
    vmem = pltpu.VMEM
    return pl.pallas_call(
        functools.partial(fused_kernel, seq_size),
        out_shape=vmem(latents.shape, half),
        in_specs=[anywhere] * 7,
        out_specs=pl.BlockSpec(memory_space=pltpu.VMEM),
        scratch_shapes=[
            pltpu.SMEM(timestep.shape, jnp.int32),
            vmem(latents.shape, half),
            vmem((3, time_table.shape[0], width), full),
            vmem((3, blocks, width), full),
            vmem(norm_gains.shape, full),
            vmem((blocks, heads, packed, width), half),
            vmem(out_weight.shape, half),
            vmem((4, pixels, width), half),
            vmem((heads, packed, tokens), full),
            vmem((heads * head_dim, tokens), full),
            vmem((4, seq_size, tile, width), full),
            vmem((seq_size, 4, tile, width), full),
            vmem((2, seq_size, tile, width), half),
            vmem((2, seq_size, tile, width), half),
            vmem((seq_size, 2, tile, width), half),
            vmem((seq_size, 2, tile, width), half),
            vmem((blocks, seq_size, tile, width), half),
            vmem((blocks, seq_size, tile, width), half),
            vmem((seq_size, tile, width), half),
            vmem((seq_size, tile, width), half),
            vmem((seq_size, 4, tile, width), half),
            vmem((seq_size, tile, width), half),
            vmem((seq_size, tile, width), half),
            pltpu.SemaphoreType.DMA((9,)),
            pltpu.SemaphoreType.DMA((copies,)),
            pltpu.SemaphoreType.DMA((copies,)),
        ],
        compiler_params=pltpu.CompilerParams(
            collective_id=0, has_side_effects=True, vmem_limit_bytes=67_043_328 - 160 * 1024
        ),
    )(
        timestep,
        latents,
        jnp.transpose(time_table, (1, 0, 2)),
        jnp.transpose(shift_table, (1, 0, 2)),
        jnp.transpose(qkv_weight, (0, 2, 3, 1)),
        norm_gains,
        out_weight,
    )


def chosen_body(mesh, *arrays):
    sizes = mesh.shape
    frames, pixels, _ = arrays[0].shape
    head_dim = arrays[4].shape[3] // 3
    fits = (
        sizes["head"] == 2
        and sizes["sub"] == 2
        and frames == 1
        and sizes["seq"] > 1
        and sizes["seq"] & (sizes["seq"] - 1) == 0
        and pixels % (16 * sizes["seq"]) == 0
        and pixels % 64 == 0
        and head_dim % 8 == 0
    )
    if fits:
        return fused_body(sizes["seq"], *arrays)
    return body(*arrays)


def solution(mesh):
    return jax.shard_map(
        functools.partial(chosen_body, mesh),
        mesh=mesh,
        in_specs=(
            P(("grp", "seq"), ("head", "sub"), None),
            P("grp"),
            P(),
            P(),
            P(None, None, ("head", "sub"), None),
            P(),
            P(None, ("head", "sub"), None),
        ),
        out_specs=P(("grp", "seq"), ("head", "sub"), None),
        check_vma=False,
    )
```

```python
import functools

import jax
import jax.numpy as jnp
from jax import lax
from jax.experimental import pallas as pl
from jax.experimental.pallas import tpu as pltpu
from jax.sharding import PartitionSpec as P

EPSILON = 1e-06


def modulate(values, shift_row, scale_row):
    widened = values.astype(jnp.float32)
    center = jnp.mean(widened, axis=-1, keepdims=True)
    spread = jnp.mean(jnp.square(widened - center), axis=-1, keepdims=True)
    normal = (widened - center) * lax.rsqrt(spread + EPSILON)
    return (normal * (1.0 + scale_row) + shift_row).astype(jnp.bfloat16)


def rms_gain(values, gain_row):
    return (
        values
        * lax.rsqrt(jnp.mean(jnp.square(values), axis=-1, keepdims=True) + EPSILON)
        * gain_row
    )


def project(normed, weight, gain_pair):
    leading = normed.shape[:-1]
    head_count = weight.shape[1]
    head_dim = weight.shape[2] // 3
    flattened = jnp.dot(
        normed.reshape(-1, normed.shape[-1]),
        weight.reshape(weight.shape[0], -1),
        preferred_element_type=jnp.float32,
    )
    pieces = flattened.reshape(leading + (head_count, 3, head_dim))
    queries = rms_gain(pieces[..., 0, :], gain_pair[0])
    key_part = rms_gain(pieces[..., 1, :], gain_pair[1])
    return jnp.concatenate([queries, key_part, pieces[..., 2, :]], axis=-1).astype(jnp.bfloat16)


def attend(packed):
    head_dim = packed.shape[-1] // 3
    queries = packed[..., :head_dim]
    key_part = packed[..., head_dim : 2 * head_dim]
    value_part = packed[..., 2 * head_dim :]
    count = queries.shape[0]
    block = 512 if count % 512 == 0 else count
    blocks = queries.reshape((count // block, block) + queries.shape[1:])

    def one_block(query_block):
        scores = jnp.einsum(
            "qhd,khd->hqk", query_block, key_part, preferred_element_type=jnp.float32
        ) * head_dim ** (-0.5)
        exponent = jnp.exp(scores)
        weights = (exponent / jnp.sum(exponent, axis=-1, keepdims=True)).astype(jnp.bfloat16)
        return jnp.einsum(
            "hqk,khd->qhd", weights, value_part, preferred_element_type=jnp.float32
        ).astype(jnp.bfloat16)

    result = lax.map(one_block, blocks)
    return result.reshape((count,) + result.shape[2:])


def body(latents, timestep, time_table, shift_table, qkv_weight, norm_gains, out_weight):
    feature_width = latents.shape[2]
    chosen = (jnp.arange(time_table.shape[0]) == timestep[0])[:, None, None]
    shared = jnp.sum(jnp.where(chosen, time_table, 0.0), axis=0)
    modulation = shared[None] + shift_table

    def gathered_heads(normed, layer_index):
        return project(
            lax.all_gather(normed, ("head", "sub"), axis=1, tiled=True),
            qkv_weight[layer_index],
            norm_gains[layer_index],
        )

    def back_to_tokens(attended, layer_index):
        merged = attended.reshape(attended.shape[0], attended.shape[1], -1)
        all_heads = lax.all_to_all(merged, ("head", "sub"), split_axis=1, concat_axis=2, tiled=True)
        row_block = all_heads.reshape(-1, all_heads.shape[-1])
        summed = jnp.dot(
            row_block,
            lax.all_gather(out_weight[layer_index], ("head", "sub"), axis=0, tiled=True),
            preferred_element_type=jnp.float32,
        )
        return summed.reshape(all_heads.shape[0], all_heads.shape[1], feature_width)

    normed = modulate(latents, modulation[0, 0], modulation[0, 1])
    packed = gathered_heads(normed, 0)
    attended = lax.map(attend, packed)
    update = back_to_tokens(attended, 0)
    current = (latents.astype(jnp.float32) + modulation[0, 2] * update).astype(jnp.bfloat16)
    shifted_rows = lax.all_to_all(current, "seq", split_axis=1, concat_axis=0, tiled=True)
    packed = gathered_heads(modulate(shifted_rows, modulation[1, 0], modulation[1, 1]), 1)
    attended = jax.vmap(attend, in_axes=1, out_axes=1)(packed)
    update = back_to_tokens(attended, 1)
    result = (shifted_rows.astype(jnp.float32) + modulation[1, 2] * update).astype(jnp.bfloat16)
    return lax.all_to_all(result, "seq", split_axis=0, concat_axis=1, tiled=True)


MESH = pl.DeviceIdType.MESH


def contract(left, right, left_dim, right_dim):
    return lax.dot_general(
        left,
        right,
        (((left_dim,), (right_dim,)), ((), ())),
        preferred_element_type=jnp.float32,
    )


def normalize(rows, shift_row, scale_row):
    center = jnp.mean(rows, axis=-1, keepdims=True)
    moved = rows - center
    spread = jnp.mean(jnp.square(moved), axis=-1, keepdims=True)
    return (moved * lax.rsqrt(spread + EPSILON) * (1.0 + scale_row) + shift_row).astype(jnp.bfloat16)


def fused_kernel(
    seq_size,
    step_hbm,
    lat_hbm,
    time_hbm,
    shift_hbm,
    qkv_hbm,
    gain_hbm,
    proj_hbm,
    out_ref,
    step_ref,
    lat,
    time_rows,
    shift_rows,
    gain,
    wq,
    wo,
    g0,
    qkv,
    att,
    part0,
    part1,
    pair0_out,
    pair0_in,
    pair1_out,
    pair1_in,
    cross_out,
    cross_in,
    current,
    seq_out,
    g1,
    back_out,
    back_in,
    load_sem,
    send_sem,
    recv_sem,
):
    grp, seq = lax.axis_index("grp"), lax.axis_index("seq")
    head, sub = lax.axis_index("head"), lax.axis_index("sub")
    sibling = (grp, seq, head, 1 - sub)
    across = (grp, seq, 1 - head, sub)

    def partner(r):
        position = seq
        bit = 1
        while bit < seq_size:
            if r & bit:
                position = position + bit - 2 * bit * lax.rem(lax.div(seq, bit), 2)
            bit *= 2
        return position

    def along(r):
        return (grp, partner(r), head, sub)

    heads, _, width = wq.shape[1:]
    head_dim = wq.shape[2] // 3
    pixels = lat.shape[1]
    tile = pixels // seq_size
    tokens = 4 * pixels

    far_first = list(range(seq_size - 1, 0, -1))
    order = far_first + [0]
    place = {r: i for i, r in enumerate([0] + far_first)}

    loads = []
    for i, (source, target) in enumerate(
        [
            (lat_hbm, lat),
            (time_hbm, time_rows),
            (shift_hbm, shift_rows),
            (gain_hbm, gain),
            (qkv_hbm.at[0], wq.at[0]),
            (proj_hbm.at[0], wo.at[0]),
            (qkv_hbm.at[1], wq.at[1]),
            (proj_hbm.at[1], wo.at[1]),
            (step_hbm, step_ref),
        ]
    ):
        load = pltpu.make_async_copy(source, target, load_sem.at[i])
        load.start()
        loads.append(load)

    barrier = pltpu.get_barrier_semaphore()
    peers = [sibling, across] + [along(r) for r in range(1, seq_size)]
    for peer in peers:
        pl.semaphore_signal(barrier, inc=1, device_id=peer, device_id_type=MESH)

    started = []

    def send(source, target, device):
        i = len(started)
        copy = pltpu.make_async_remote_copy(
            src_ref=source,
            dst_ref=target,
            send_sem=send_sem.at[i],
            recv_sem=recv_sem.at[i],
            device_id=device,
            device_id_type=MESH,
        )
        copy.start()
        started.append(copy)
        return copy

    for load in loads[:4] + loads[8:]:
        load.wait()
    step = step_ref[0]

    def modulation(block, j):
        return time_rows[j, pl.ds(step, 1), :] + shift_rows[j, pl.ds(block, 1), :]

    def chunk_rows(r):
        start = partner(r) * tile
        return pl.ds(pl.multiple_of(start, tile), tile)

    shift0, scale0, gate0 = (modulation(0, j) for j in range(3))
    for r in range(seq_size):
        rows = lat[0, chunk_rows(r), :].astype(jnp.float32)
        g0[0, pl.ds(r * tile, tile), :] = normalize(rows, shift0, scale0)

    diagonal = lax.broadcasted_iota(jnp.int32, (head_dim, head_dim), 0) == lax.broadcasted_iota(
        jnp.int32, (head_dim, head_dim), 1
    )

    def gain_column(block, which):
        row = gain[block, pl.ds(which, 1), :]
        return jnp.sum(jnp.where(diagonal, row, 0.0), axis=1, keepdims=True)

    pl.semaphore_wait(barrier, len(peers))

    half = pixels // 2
    halves = [pl.ds(0, half), pl.ds(half, half)]
    cross = [send(g0.at[0, part], g0.at[2, part], across) for part in halves]
    pair = send(g0.at[0], g0.at[1], sibling)

    def project_block(block, values, side):
        lanes = pl.ds(side * (tokens // 2), tokens // 2)
        for h in range(heads):
            flat = contract(wq[block, h], values, 1, 1)
            for j in range(3):
                piece = flat[j * head_dim : (j + 1) * head_dim]
                if j < 2:
                    mean = jnp.mean(jnp.square(piece), axis=0, keepdims=True)
                    piece = piece * lax.rsqrt(mean + EPSILON) * gains[block][j]
                qkv[h, pl.ds(j * head_dim, head_dim), lanes] = piece

    gains = [[gain_column(block, j) for j in range(2)] for block in range(2)]
    loads[4].wait()
    pair.wait_recv()
    project_block(0, g0[0:2].reshape(2 * pixels, width), 0)
    forwarded = []
    for part, copy in zip(halves, cross):
        copy.wait_recv()
        forwarded.append(send(g0.at[2, part], g0.at[3, part], sibling))
    for copy in forwarded:
        copy.wait_recv()
    project_block(0, g0[2:4].reshape(2 * pixels, width), 1)

    scale = head_dim ** (-0.5)

    for h in range(heads):
        queries = qkv[h, 0:head_dim].astype(jnp.bfloat16)
        keys = qkv[h, head_dim : 2 * head_dim].astype(jnp.bfloat16)
        values = qkv[h, 2 * head_dim : 3 * head_dim].astype(jnp.bfloat16)
        exponent = jnp.exp(contract(keys, queries, 0, 0) * scale)
        total = jnp.sum(exponent, axis=0, keepdims=True)
        mixed = contract(values, exponent.astype(jnp.bfloat16), 1, 0)
        att[pl.ds(h * head_dim, head_dim)] = mixed / total

    def project_out(block, side, part):
        lanes = pl.ds(side * (tokens // 2), tokens // 2)
        partial = contract(att[:, lanes].astype(jnp.bfloat16), wo[block], 0, 0)
        first = side * (part.shape[0] // 2)
        part[pl.ds(first, part.shape[0] // 2)] = partial.reshape(
            (part.shape[0] // 2,) + part.shape[1:]
        )

    loads[5].wait()
    project_out(0, 1, part0)
    far_pairs = {}
    for r in order:
        pair0_out[1, r] = part0[3, r].astype(jnp.bfloat16)
        far_pairs[r] = send(pair0_out.at[1, r], pair0_in.at[1, r], sibling)
    project_out(0, 0, part0)
    pair0_out[0] = part0[1].astype(jnp.bfloat16)
    near_pair = send(pair0_out.at[0], pair0_in.at[0], sibling)
    crosses = {}
    for r in order:
        far_pairs[r].wait_recv()
        summed = part0[2, r] + pair0_in[1, r].astype(jnp.float32)
        cross_out[0, r] = summed.astype(jnp.bfloat16)
        crosses[r] = send(cross_out.at[0, r], cross_in.at[0, r], across)
    near_pair.wait_recv()
    shift1, scale1, gate1 = (modulation(1, j) for j in range(3))
    moves = {}
    for r in order:
        crosses[r].wait_recv()
        update = (
            part0[0, r]
            + pair0_in[0, r].astype(jnp.float32)
            + cross_in[0, r].astype(jnp.float32)
        )
        rows = (lat[0, chunk_rows(r), :].astype(jnp.float32) + gate0 * update).astype(jnp.bfloat16)
        current[r] = rows
        normed = normalize(rows.astype(jnp.float32), shift1, scale1)
        if r:
            seq_out[r] = normed
            moves[r] = send(seq_out.at[r], g1.at[place[r], 0], along(r))
        else:
            g1[0, 0] = normed

    loads[6].wait()
    by_place = [0] + far_first
    gathered = []

    def spread(i):
        gathered.append(
            (
                send(g1.at[i, 0], g1.at[i, 2], across),
                send(g1.at[i, 0], g1.at[i, 1], sibling),
            )
        )

    relayed = []

    def relay(i):
        gathered[i][0].wait_recv()
        relayed.append(send(g1.at[i, 2], g1.at[i, 3], sibling))

    middle = seq_size // 2
    spread(0)
    for i in range(1, seq_size):
        moves[by_place[i]].wait_recv()
        spread(i)
    for i in range(seq_size):
        relay(i)

    def ready(places):
        for i in places:
            gathered[i][1].wait_recv()
            relayed[i].wait_recv()

    ready(range(middle))
    project_block(1, g1[0:middle].reshape(2 * pixels, width), 0)
    ready(range(middle, seq_size))
    project_block(1, g1[middle:seq_size].reshape(2 * pixels, width), 1)

    for h in range(heads):
        queries, keys, values = (
            qkv[h, pl.ds(j * head_dim, head_dim)].astype(jnp.bfloat16).astype(jnp.float32)
            for j in range(3)
        )
        total = jnp.zeros((1, tokens), jnp.float32)
        mixed = jnp.zeros((head_dim, tokens), jnp.float32)
        for r in range(seq_size):
            turn = r * 4 * tile
            turned_keys = pltpu.roll(keys, turn, 1) if r else keys
            turned_values = pltpu.roll(values, turn, 1) if r else values
            exponent = jnp.exp(jnp.sum(queries * turned_keys, axis=0, keepdims=True) * scale)
            total = total + exponent
            mixed = mixed + exponent * turned_values
        att[pl.ds(h * head_dim, head_dim)] = mixed / total

    loads[7].wait()
    pairs, crosses = {}, {}
    for side in range(2):
        project_out(1, side, part1)
        for i in range(side * middle, (side + 1) * middle):
            r = by_place[i]
            pair1_out[r, 0] = part1[i, 1].astype(jnp.bfloat16)
            pair1_out[r, 1] = part1[i, 3].astype(jnp.bfloat16)
            pairs[r] = send(pair1_out.at[r], pair1_in.at[r], sibling)
    for r in order:
        pairs[r].wait_recv()
        summed = part1[place[r], 2] + pair1_in[r, 1].astype(jnp.float32)
        cross_out[1, r] = summed.astype(jnp.bfloat16)
        crosses[r] = send(cross_out.at[1, r], cross_in.at[1, r], across)
    returns = {}
    for r in order:
        crosses[r].wait_recv()
        update = (
            part1[place[r], 0]
            + pair1_in[r, 0].astype(jnp.float32)
            + cross_in[1, r].astype(jnp.float32)
        )
        if r:
            back_out[r] = update.astype(jnp.bfloat16)
            returns[r] = send(back_out.at[r], back_in.at[r], along(r))
        else:
            rows = current[r].astype(jnp.float32) + gate1 * update
            out_ref[0, chunk_rows(r), :] = rows.astype(jnp.bfloat16)
    for r in far_first:
        returns[r].wait_recv()
        rows = current[r].astype(jnp.float32) + gate1 * back_in[r].astype(jnp.float32)
        out_ref[0, chunk_rows(r), :] = rows.astype(jnp.bfloat16)
    for copy in started:
        copy.wait_send()


def fused_body(seq_size, latents, timestep, time_table, shift_table, qkv_weight, norm_gains, out_weight):
    _, pixels, width = latents.shape
    blocks, _, heads, packed = qkv_weight.shape
    head_dim = packed // 3
    tile = pixels // seq_size
    tokens = 4 * pixels
    copies = 6 + 4 * seq_size + 2 * (seq_size - 1) + 3 * seq_size
    anywhere = pl.BlockSpec(memory_space=pl.ANY)
    half, full = jnp.bfloat16, jnp.float32
    vmem = pltpu.VMEM
    return pl.pallas_call(
        functools.partial(fused_kernel, seq_size),
        out_shape=vmem(latents.shape, half),
        in_specs=[anywhere] * 7,
        out_specs=pl.BlockSpec(memory_space=pltpu.VMEM),
        scratch_shapes=[
            pltpu.SMEM(timestep.shape, jnp.int32),
            vmem(latents.shape, half),
            vmem((3, time_table.shape[0], width), full),
            vmem((3, blocks, width), full),
            vmem(norm_gains.shape, full),
            vmem((blocks, heads, packed, width), half),
            vmem(out_weight.shape, half),
            vmem((4, pixels, width), half),
            vmem((heads, packed, tokens), full),
            vmem((heads * head_dim, tokens), full),
            vmem((4, seq_size, tile, width), full),
            vmem((seq_size, 4, tile, width), full),
            vmem((2, seq_size, tile, width), half),
            vmem((2, seq_size, tile, width), half),
            vmem((seq_size, 2, tile, width), half),
            vmem((seq_size, 2, tile, width), half),
            vmem((blocks, seq_size, tile, width), half),
            vmem((blocks, seq_size, tile, width), half),
            vmem((seq_size, tile, width), half),
            vmem((seq_size, tile, width), half),
            vmem((seq_size, 4, tile, width), half),
            vmem((seq_size, tile, width), half),
            vmem((seq_size, tile, width), half),
            pltpu.SemaphoreType.DMA((9,)),
            pltpu.SemaphoreType.DMA((copies,)),
            pltpu.SemaphoreType.DMA((copies,)),
        ],
        compiler_params=pltpu.CompilerParams(
            collective_id=0, has_side_effects=True, vmem_limit_bytes=67_043_328 - 160 * 1024
        ),
    )(
        timestep,
        latents,
        jnp.transpose(time_table, (1, 0, 2)),
        jnp.transpose(shift_table, (1, 0, 2)),
        jnp.transpose(qkv_weight, (0, 2, 3, 1)),
        norm_gains,
        out_weight,
    )


def chosen_body(mesh, *arrays):
    sizes = mesh.shape
    frames, pixels, _ = arrays[0].shape
    head_dim = arrays[4].shape[3] // 3
    fits = (
        sizes["head"] == 2
        and sizes["sub"] == 2
        and frames == 1
        and sizes["seq"] > 1
        and sizes["seq"] & (sizes["seq"] - 1) == 0
        and pixels % (16 * sizes["seq"]) == 0
        and pixels % 64 == 0
        and head_dim % 8 == 0
    )
    if fits:
        return fused_body(sizes["seq"], *arrays)
    return body(*arrays)


def solution(mesh):
    return jax.shard_map(
        functools.partial(chosen_body, mesh),
        mesh=mesh,
        in_specs=(
            P(("grp", "seq"), ("head", "sub"), None),
            P("grp"),
            P(),
            P(),
            P(None, None, ("head", "sub"), None),
            P(),
            P(None, ("head", "sub"), None),
        ),
        out_specs=P(("grp", "seq"), ("head", "sub"), None),
        check_vma=False,
    )
```
